32 devices in a mesh: row: 8 (over y, x, core), col: 4 (over z).
Axes of the slice: x: 2, y: 2, z: 4, core: 2. Of those that a mesh axis runs over, the one named last changes fastest.
Arguments:
- window_rows: bfloat16 [1024, 65536], P('row', 'col'), may hold values from -6 to 6
- omega_cols: bfloat16 [512, 1024], P(None, 'row'), may hold values from -0.1875 to 0.1875
- psi_rows: bfloat16 [65536, 1024], P(('col', 'row')), may hold values from -0.046875 to 0.046875
- upsilon_rows: bfloat16 [65536, 2048], P(('col', 'row')), may hold values from -0.046875 to 0.046875
- phi_cols: bfloat16 [2048, 1024], P(None, 'row'), may hold values from -0.1875 to 0.1875
- range_old: float32 [512, 65536], P(None, ('col', 'row')), may hold values from -6 to 6
- core_old: float32 [2048, 2048], P('row', 'col'), may hold values from -6 to 6
Outputs:
- range_sketch: float32 [512, 65536], P(None, ('col', 'row'))
- corange_sketch: float32 [1024, 1024], P('row', 'col')
- core_sketch: float32 [2048, 2048], P('row', 'col')
The draws below stay inside these ranges and needn't reach their ends.
All inputs are finite; a program needn't handle non-finite values.
Results may differ from the reference program's by a relative error of at most 0.0022.
Values may be sent and summed in bfloat16 or wider, within the bound.
A program may use at most 128 MiB of HBM per device.

```python
import jax
import jax.numpy as jnp

NCOLS = 65536
K = 512
L = 1024
S = 2048
WINDOW = 1024


def with_spikes(result, own_key, source, target, blocks, factor):
    def block_of(axis_at):
        return (jnp.arange(result.shape[axis_at]) // (result.shape[axis_at] // blocks)).reshape((-1,) + (1,) * (result.ndim - 1 - axis_at))

    first = jax.random.permutation(own_key, blocks)[block_of(target)]
    far = (block_of(target) + blocks // 2) % blocks
    return jnp.where((block_of(source) == first) | (block_of(source) == far), factor * result, result)


def block_levels(rng, shape, split, least, largest):
    factor_of = 1.0
    for position, parts in split:
        heights = jax.random.uniform(jax.random.fold_in(jax.random.fold_in(rng, 6), position), (parts,), jnp.float32, least / len(split), largest / len(split))
        factor_of = factor_of * jnp.repeat(jnp.exp(heights), shape[position] // parts).reshape((-1,) + (1,) * (len(shape) - 1 - position))
    return factor_of


def gaussian(own_key, extent, deviation, most, shards=(), kind=jnp.bfloat16):
    result = deviation * jax.random.normal(own_key, extent, jnp.float32)
    if shards:
        result = result * block_levels(own_key, extent, shards, -0.22, 0.18)
    return jnp.clip(result, -most, most).astype(kind)


def bell_draw_with(key, dims, deviation, bound, pieces, heavy, dtype=jnp.bfloat16):
    result = deviation * jax.random.normal(key, dims, jnp.float32)
    if pieces:
        result = result * block_levels(key, dims, pieces, -0.22, 0.18)
    return jnp.clip(with_spikes(result, jax.random.fold_in(key, 3), *heavy), -bound, bound).astype(dtype)


def setup_inputs(seed: int = 0) -> dict:
    key_list = jax.random.split(jax.random.key(seed), 8)
    return {
        "window_rows": gaussian(key_list[0], (WINDOW, NCOLS), 1.0, 6.0, ((0, 8), (1, 4))),
        "omega_cols": gaussian(key_list[1], (K, WINDOW), WINDOW ** -0.5, 0.1875, ((1, 8),)),
        "psi_rows": bell_draw_with(key_list[2], (NCOLS, L), NCOLS ** -0.5, 0.046875, ((0, 32),), (0, 1, 32, 2.75)),
        "upsilon_rows": bell_draw_with(key_list[3], (NCOLS, S), NCOLS ** -0.5, 0.046875, ((0, 32),), (0, 1, 32, 2.75)),
        "phi_cols": gaussian(key_list[4], (S, WINDOW), WINDOW ** -0.5, 0.1875, ((1, 8),)),
        "range_old": gaussian(key_list[5], (K, NCOLS), 1.0, 6.0, ((1, 32),), jnp.float32),
        "core_old": gaussian(key_list[6], (S, S), 1.0, 6.0, ((0, 8), (1, 4)), jnp.float32),
    }


def reference(window_rows, omega_cols, psi_rows, upsilon_rows, phi_cols, range_old, core_old):
    range_sketch = range_old + jnp.dot(omega_cols, window_rows, preferred_element_type=jnp.float32)
    corange_sketch = jnp.dot(window_rows, psi_rows, preferred_element_type=jnp.float32)
    sketched = jnp.dot(window_rows, upsilon_rows, preferred_element_type=jnp.float32).astype(jnp.bfloat16)
    core_sketch = core_old + jnp.dot(phi_cols, sketched, preferred_element_type=jnp.float32)
    return range_sketch, corange_sketch, core_sketch
```

```python
import functools

import jax
import jax.numpy as jnp
from jax import lax
from jax.experimental import pallas as pl
from jax.experimental.pallas import tpu as pltpu
from jax.sharding import PartitionSpec as P

MESH = pl.DeviceIdType.MESH
LIMIT = 60 * 1024 * 1024


def greet(peers):
    barrier = pltpu.get_barrier_semaphore()
    for peer in peers:
        pl.semaphore_signal(barrier, inc=1, device_id=peer, device_id_type=MESH)
    pl.semaphore_wait(barrier, len(peers))


def send(src, dst, send_sem, recv_sem, peer):
    copy = pltpu.make_async_remote_copy(
        src_ref=src, dst_ref=dst, send_sem=send_sem, recv_sem=recv_sem, device_id=peer, device_id_type=MESH
    )
    copy.start()
    return copy


def exchange(n, window, phi, relaid, phi_all, keep_w, keep_p, send_sem, recv_sem, local_sem):
    me = lax.axis_index("row")
    rows, width = window.shape[0], relaid.shape[1]
    core_rows, depth = phi_all.shape[0], phi.shape[1]
    peers = [lax.rem(me + d, n) for d in range(1, n)]
    greet([{"row": p} for p in peers])
    copies = []
    for d, p in enumerate(peers):
        copies.append(send(
            window.at[:, pl.ds(pl.multiple_of(p * width, width), width)],
            relaid.at[pl.ds(pl.multiple_of(me * rows, rows), rows), :],
            send_sem.at[0, d], recv_sem.at[0, d], {"row": p}))
    for d, p in enumerate(peers):
        copies.append(send(
            phi.at[pl.ds(pl.multiple_of(p * core_rows, core_rows), core_rows), :],
            phi_all.at[:, pl.ds(pl.multiple_of(me * depth, depth), depth)],
            send_sem.at[1, d], recv_sem.at[1, d], {"row": p}))
    ins = (
        pltpu.make_async_copy(window.at[:, pl.ds(pl.multiple_of(me * width, width), width)], keep_w, local_sem.at[0]),
        pltpu.make_async_copy(phi.at[pl.ds(pl.multiple_of(me * core_rows, core_rows), core_rows), :], keep_p, local_sem.at[1]),
    )
    for c in ins:
        c.start()
    for c in ins:
        c.wait()
    outs = (
        pltpu.make_async_copy(keep_w, relaid.at[pl.ds(pl.multiple_of(me * rows, rows), rows), :], local_sem.at[2]),
        pltpu.make_async_copy(keep_p, phi_all.at[:, pl.ds(pl.multiple_of(me * depth, depth), depth)], local_sem.at[3]),
    )
    for c in outs:
        c.start()
    for c in outs:
        c.wait()
    for c in copies:
        c.wait()


def reduce_kernel(n, m, sk, co, gathered, co_out, *scratch):
    (acc_sk, acc_co, *recv), rest = scratch[:2 + 2 * (n.bit_length() - 1)], scratch[2 + 2 * (n.bit_length() - 1):]
    fin_sk, fin_co, z_sk, z_co, mine, load_sem, ss, rs, zs, zr, gs, gr, ls = rest
    levels = n.bit_length() - 1
    me, c = lax.axis_index("row"), lax.axis_index("col")
    bits = [(me // (1 << b)) % 2 for b in range(levels)]
    partner = [{"row": me + (1 - 2 * bits[b]) * (1 << b)} for b in range(levels)]
    row_peers = [lax.rem(me + d, n) for d in range(1, n)]
    col_peers = [lax.rem(c + d, m) for d in range(1, m)]
    greet([{"row": p} for p in row_peers] + [{"col": p} for p in col_peers])

    pieces = []
    low, high = list(range(1, levels)), list(range(levels - 1, 0, -1))
    for k, (src, acc, fin) in enumerate(((sk, acc_sk, fin_sk), (co, acc_co, fin_co))):
        half = src.shape[-1] // 2
        for h, order in enumerate((low, high)):
            pieces.append((src, acc, recv[k::2], fin, pl.ds(h * half, half), order))

    copies = []
    first = []
    for q, (src, acc, got, fin, cols, order) in enumerate(pieces):
        mine_first = []
        for i in range(n // 2):
            mine_first.append(send(
                src.at[i, 1 - bits[0], :, cols], got[0].at[i, :, cols], ss.at[q, 0, i], rs.at[q, 0, i], partner[0]))
        first.append(mine_first)
    loads = []
    for q, (src, acc, got, fin, cols, order) in enumerate(pieces):
        load = pltpu.make_async_copy(src.at[:, bits[0], :, cols], acc.at[:, :, cols], load_sem.at[q])
        load.start()
        loads.append(load)

    live = []
    for q, (src, acc, got, fin, cols, order) in enumerate(pieces):
        loads[q].wait()
        live.append((0, n // 2, 1))
        for i in range(n // 2):
            first[q][i].wait_recv()
            acc[i, :, cols] += got[0][i, :, cols]
        copies += first[q]
        if levels > 1:
            pass

    def at(base, stride, i):
        return base + stride * i

    for step in range(levels - 1):
        started = []
        for q, (src, acc, got, fin, cols, order) in enumerate(pieces):
            base, count, stride = live[q]
            bit = bits[order[step]]
            if order is not high and order == low:
                keep = (base + stride * bit, count // 2, stride * 2)
                give = (base + stride * (1 - bit), count // 2, stride * 2)
            else:
                keep = (base + stride * (count // 2) * bit, count // 2, stride)
                give = (base + stride * (count // 2) * (1 - bit), count // 2, stride)
            sent = []
            for i in range(count // 2):
                sent.append(send(
                    acc.at[at(give[0], give[2], i), :, cols], got[step + 1].at[i, :, cols],
                    ss.at[q, step + 1, i], rs.at[q, step + 1, i], partner[order[step]]))
            started.append(sent)
            live[q] = keep
        for q, (src, acc, got, fin, cols, order) in enumerate(pieces):
            base, count, stride = live[q]
            for i in range(count):
                started[q][i].wait_recv()
                j = at(base, stride, i)
                acc[j, :, cols] += got[step + 1][i, :, cols]
            copies += started[q]
    for q, (src, acc, got, fin, cols, order) in enumerate(pieces):
        fin[:, cols] = acc[live[q][0], :, cols]

    across = []
    for k, (fin, z) in enumerate(((fin_sk, z_sk), (fin_co, z_co))):
        width = z.shape[-1]
        across.append([
            send(fin.at[:, pl.ds(pl.multiple_of(p * width, width), width)], z.at[d], zs.at[k, d], zr.at[k, d], {"col": p})
            for d, p in enumerate(col_peers)])
    sums = []
    for k, (fin, z) in enumerate(((fin_sk, z_sk), (fin_co, z_co))):
        width = z.shape[-1]
        own = pl.ds(pl.multiple_of(c * width, width), width)
        for copy in across[k]:
            copy.wait_recv()
        total = fin[:, own]
        for d in range(m - 1):
            total = total + z[d]
        if k == 0:
            mine[...] = total.astype(mine.dtype)
            rows = mine.shape[0]
            place = gathered.at[pl.ds(pl.multiple_of(me * rows, rows), rows), :]
            spread = [
                send(mine, place, gs.at[d], gr.at[d], {"row": p}) for d, p in enumerate(row_peers)]
            put = pltpu.make_async_copy(mine, place, ls)
            put.start()
        else:
            co_out[...] = total
        copies += across[k]
    put.wait()
    for copy in spread:
        copy.wait()
    for copy in copies:
        copy.wait_send()


def shards(n, m, window_rows, omega_cols, psi_rows, upsilon_rows, phi_cols, range_old, core_old):
    any_space = pl.BlockSpec(memory_space=pl.ANY)
    vmem = pl.BlockSpec(memory_space=pltpu.VMEM)
    dma = pltpu.SemaphoreType.DMA
    rows, wide = window_rows.shape
    own = wide // n
    core_rows = phi_cols.shape[0] // n
    bf16, f32 = jnp.bfloat16, jnp.float32
    relaid, phi_all = pl.pallas_call(
        functools.partial(exchange, n),
        out_shape=(jax.ShapeDtypeStruct((rows * n, own), bf16), jax.ShapeDtypeStruct((core_rows, rows * n), bf16)),
        in_specs=[any_space] * 2,
        out_specs=(any_space, any_space),
        scratch_shapes=[
            pltpu.VMEM((rows, own), bf16), pltpu.VMEM((core_rows, rows), bf16),
            dma((2, n - 1)), dma((2, n - 1)), dma((4,)),
        ],
        compiler_params=pltpu.CompilerParams(collective_id=0, has_side_effects=True),
        name="exchange",
    )(window_rows, phi_cols)
    omega = lax.all_gather(omega_cols, "row", axis=1, tiled=True)
    core_part = jnp.dot(relaid, upsilon_rows, preferred_element_type=f32)
    co_part = jnp.dot(relaid, psi_rows, preferred_element_type=f32)
    s, l = core_part.shape[1], co_part.shape[1]
    levels = n.bit_length() - 1
    scratch = [pltpu.VMEM((n // 2, rows, s), f32), pltpu.VMEM((n // 2, rows, l), f32)]
    for b in range(levels):
        scratch += [pltpu.VMEM((n >> (b + 1), rows, s), f32), pltpu.VMEM((n >> (b + 1), rows, l), f32)]
    scratch += [
        pltpu.VMEM((rows, s), f32), pltpu.VMEM((rows, l), f32),
        pltpu.VMEM((m - 1, rows, s // m), f32), pltpu.VMEM((m - 1, rows, l // m), f32),
        pltpu.VMEM((rows, s // m), bf16), dma((4,)),
        dma((4, levels, n // 2)), dma((4, levels, n // 2)),
        dma((2, m - 1)), dma((2, m - 1)), dma((n - 1,)), dma((n - 1,)), dma,
    ]
    gathered, corange_sketch = pl.pallas_call(
        functools.partial(reduce_kernel, n, m),
        out_shape=(jax.ShapeDtypeStruct((rows * n, s // m), bf16), jax.ShapeDtypeStruct((rows, l // m), f32)),
        in_specs=[any_space] * 2,
        out_specs=(any_space, vmem),
        scratch_shapes=scratch,
        compiler_params=pltpu.CompilerParams(collective_id=1, has_side_effects=True, vmem_limit_bytes=LIMIT),
        name="reduce",
    )(core_part.reshape(n // 2, 2, rows, s), co_part.reshape(n // 2, 2, rows, l))
    range_sketch = range_old + jnp.dot(omega, relaid, preferred_element_type=f32)
    core_sketch = core_old + jnp.dot(phi_all, gathered, preferred_element_type=f32)
    return (range_sketch, corange_sketch, core_sketch)


def solution(mesh):
    placed = (
        P("row", "col"),
        P(None, "row"),
        P(("col", "row"), None),
        P(("col", "row"), None),
        P(None, "row"),
        P(None, ("col", "row")),
        P("row", "col"),
    )
    return jax.shard_map(
        functools.partial(shards, mesh.shape["row"], mesh.shape["col"]),
        mesh=mesh,
        in_specs=placed,
        out_specs=(P(None, ("col", "row")), P("row", "col"), P("row", "col")),
        check_vma=False,
    )
```

```python
import functools

import jax
import jax.numpy as jnp
from jax import lax
from jax.experimental import pallas as pl
from jax.experimental.pallas import tpu as pltpu
from jax.sharding import PartitionSpec as P

MESH = pl.DeviceIdType.MESH
LIMIT = 60 * 1024 * 1024


def greet(peers):
    barrier = pltpu.get_barrier_semaphore()
    for peer in peers:
        pl.semaphore_signal(barrier, inc=1, device_id=peer, device_id_type=MESH)
    pl.semaphore_wait(barrier, len(peers))


def send(src, dst, send_sem, recv_sem, peer):
    copy = pltpu.make_async_remote_copy(
        src_ref=src, dst_ref=dst, send_sem=send_sem, recv_sem=recv_sem, device_id=peer, device_id_type=MESH
    )
    copy.start()
    return copy


def exchange(n, window, phi, relaid, phi_all, keep_w, keep_p, send_sem, recv_sem, local_sem):
    me = lax.axis_index("row")
    rows, width = window.shape[0], relaid.shape[1]
    core_rows, depth = phi_all.shape[0], phi.shape[1]
    peers = [lax.rem(me + d, n) for d in range(1, n)]
    greet([{"row": p} for p in peers])
    copies = []
    for d, p in enumerate(peers):
        copies.append(send(
            window.at[:, pl.ds(pl.multiple_of(p * width, width), width)],
            relaid.at[pl.ds(pl.multiple_of(me * rows, rows), rows), :],
            send_sem.at[0, d], recv_sem.at[0, d], {"row": p}))
    for d, p in enumerate(peers):
        copies.append(send(
            phi.at[pl.ds(pl.multiple_of(p * core_rows, core_rows), core_rows), :],
            phi_all.at[:, pl.ds(pl.multiple_of(me * depth, depth), depth)],
            send_sem.at[1, d], recv_sem.at[1, d], {"row": p}))
    ins = (
        pltpu.make_async_copy(window.at[:, pl.ds(pl.multiple_of(me * width, width), width)], keep_w, local_sem.at[0]),
        pltpu.make_async_copy(phi.at[pl.ds(pl.multiple_of(me * core_rows, core_rows), core_rows), :], keep_p, local_sem.at[1]),
    )
    for c in ins:
        c.start()
    for c in ins:
        c.wait()
    outs = (
        pltpu.make_async_copy(keep_w, relaid.at[pl.ds(pl.multiple_of(me * rows, rows), rows), :], local_sem.at[2]),
        pltpu.make_async_copy(keep_p, phi_all.at[:, pl.ds(pl.multiple_of(me * depth, depth), depth)], local_sem.at[3]),
    )
    for c in outs:
        c.start()
    for c in outs:
        c.wait()
    for c in copies:
        c.wait()


def reduce_kernel(n, m, sk, co, gathered, co_out, *scratch):
    (acc_sk, acc_co, *recv), rest = scratch[:2 + 2 * (n.bit_length() - 1)], scratch[2 + 2 * (n.bit_length() - 1):]
    fin_sk, fin_co, z_sk, z_co, mine, load_sem, ss, rs, zs, zr, gs, gr, ls = rest
    levels = n.bit_length() - 1
    me, c = lax.axis_index("row"), lax.axis_index("col")
    bits = [(me // (1 << b)) % 2 for b in range(levels)]
    partner = [{"row": me + (1 - 2 * bits[b]) * (1 << b)} for b in range(levels)]
    row_peers = [lax.rem(me + d, n) for d in range(1, n)]
    col_peers = [lax.rem(c + d, m) for d in range(1, m)]
    greet([{"row": p} for p in row_peers] + [{"col": p} for p in col_peers])

    pieces = []
    low, high = list(range(1, levels)), list(range(levels - 1, 0, -1))
    for k, (src, acc, fin) in enumerate(((sk, acc_sk, fin_sk), (co, acc_co, fin_co))):
        half = src.shape[-1] // 2
        for h, order in enumerate((low, high)):
            pieces.append((src, acc, recv[k::2], fin, pl.ds(h * half, half), order))

    copies = []
    first = []
    for q, (src, acc, got, fin, cols, order) in enumerate(pieces):
        first.append([
            send(src.at[i, 1 - bits[0], :, cols], got[0].at[i, :, cols], ss.at[q, 0, i], rs.at[q, 0, i], partner[0])
            for i in range(n // 2)])
    loads = []
    for q, (src, acc, got, fin, cols, order) in enumerate(pieces):
        load = pltpu.make_async_copy(src.at[:, bits[0], :, cols], acc.at[:, :, cols], load_sem.at[q])
        load.start()
        loads.append(load)

    live = [(0, n // 2, 1)] * 4
    started = [None] * 4

    def pair(q):
        src, acc, got, fin, cols, order = pieces[q]
        loads[q].wait()
        for i in range(n // 2):
            first[q][i].wait_recv()
            acc[i, :, cols] += got[0][i, :, cols]
        copies.extend(first[q])

    def give(q, step):
        src, acc, got, fin, cols, order = pieces[q]
        base, count, stride = live[q]
        bit, half = bits[order[step]], count // 2
        if order is low:
            live[q] = (base + stride * bit, half, stride * 2)
            start, jump = base + stride * (1 - bit), stride * 2
        else:
            live[q] = (base + stride * half * bit, half, stride)
            start, jump = base + stride * half * (1 - bit), stride
        started[q] = [
            send(acc.at[start + jump * i, :, cols], got[step + 1].at[i, :, cols],
                 ss.at[q, step + 1, i], rs.at[q, step + 1, i], partner[order[step]])
            for i in range(half)]

    def take(q, step):
        src, acc, got, fin, cols, order = pieces[q]
        base, count, stride = live[q]
        for i in range(count):
            started[q][i].wait_recv()
            if step == levels - 2:
                fin[:, cols] = acc[base + stride * i, :, cols] + got[step + 1][i, :, cols]
            else:
                acc[base + stride * i, :, cols] += got[step + 1][i, :, cols]
        copies.extend(started[q])

    def cross(k):
        fin, z = ((fin_sk, z_sk), (fin_co, z_co))[k]
        width = z.shape[-1]
        return [
            send(fin.at[:, pl.ds(pl.multiple_of(p * width, width), width)], z.at[d], zs.at[k, d], zr.at[k, d], {"col": p})
            for d, p in enumerate(col_peers)]

    for q in (0, 1):
        pair(q)
        give(q, 0)
    for q in (2, 3):
        pair(q)
    for step in range(levels - 1):
        for q in (0, 1):
            take(q, step)
            if step < levels - 2:
                give(q, step + 1)
        if step == max(levels - 3, 0):
            for q in (2, 3):
                give(q, 0)
    across = [cross(0)]
    for step in range(levels - 1):
        for q in (2, 3):
            take(q, step)
            if step < levels - 2:
                give(q, step + 1)
    across.append(cross(1))
    for k, (fin, z) in enumerate(((fin_sk, z_sk), (fin_co, z_co))):
        width = z.shape[-1]
        own = pl.ds(pl.multiple_of(c * width, width), width)
        for copy in across[k]:
            copy.wait_recv()
        total = fin[:, own]
        for d in range(m - 1):
            total = total + z[d]
        if k == 0:
            mine[...] = total.astype(mine.dtype)
            rows = mine.shape[0]
            place = gathered.at[pl.ds(pl.multiple_of(me * rows, rows), rows), :]
            spread = [
                send(mine, place, gs.at[d], gr.at[d], {"row": p}) for d, p in enumerate(row_peers)]
            put = pltpu.make_async_copy(mine, place, ls)
            put.start()
        else:
            co_out[...] = total
        copies += across[k]
    put.wait()
    for copy in spread:
        copy.wait()
    for copy in copies:
        copy.wait_send()


def shards(n, m, window_rows, omega_cols, psi_rows, upsilon_rows, phi_cols, range_old, core_old):
    any_space = pl.BlockSpec(memory_space=pl.ANY)
    vmem = pl.BlockSpec(memory_space=pltpu.VMEM)
    dma = pltpu.SemaphoreType.DMA
    rows, wide = window_rows.shape
    own = wide // n
    core_rows = phi_cols.shape[0] // n
    bf16, f32 = jnp.bfloat16, jnp.float32
    relaid, phi_all = pl.pallas_call(
        functools.partial(exchange, n),
        out_shape=(jax.ShapeDtypeStruct((rows * n, own), bf16), jax.ShapeDtypeStruct((core_rows, rows * n), bf16)),
        in_specs=[any_space] * 2,
        out_specs=(any_space, any_space),
        scratch_shapes=[
            pltpu.VMEM((rows, own), bf16), pltpu.VMEM((core_rows, rows), bf16),
            dma((2, n - 1)), dma((2, n - 1)), dma((4,)),
        ],
        compiler_params=pltpu.CompilerParams(collective_id=0, has_side_effects=True),
        name="exchange",
    )(window_rows, phi_cols)
    relaid, omega_cols = lax.optimization_barrier((relaid, omega_cols))
    omega = lax.all_gather(omega_cols, "row", axis=1, tiled=True)
    core_part = jnp.dot(relaid, upsilon_rows, preferred_element_type=f32)
    co_part = jnp.dot(relaid, psi_rows, preferred_element_type=f32)
    s, l = core_part.shape[1], co_part.shape[1]
    levels = n.bit_length() - 1
    scratch = [pltpu.VMEM((n // 2, rows, s), f32), pltpu.VMEM((n // 2, rows, l), f32)]
    for b in range(levels):
        scratch += [pltpu.VMEM((n >> (b + 1), rows, s), f32), pltpu.VMEM((n >> (b + 1), rows, l), f32)]
    scratch += [
        pltpu.VMEM((rows, s), f32), pltpu.VMEM((rows, l), f32),
        pltpu.VMEM((m - 1, rows, s // m), f32), pltpu.VMEM((m - 1, rows, l // m), f32),
        pltpu.VMEM((rows, s // m), bf16), dma((4,)),
        dma((4, levels, n // 2)), dma((4, levels, n // 2)),
        dma((2, m - 1)), dma((2, m - 1)), dma((n - 1,)), dma((n - 1,)), dma,
    ]
    gathered, corange_sketch = pl.pallas_call(
        functools.partial(reduce_kernel, n, m),
        out_shape=(jax.ShapeDtypeStruct((rows * n, s // m), bf16), jax.ShapeDtypeStruct((rows, l // m), f32)),
        in_specs=[any_space] * 2,
        out_specs=(any_space, vmem),
        scratch_shapes=scratch,
        compiler_params=pltpu.CompilerParams(collective_id=1, has_side_effects=True, vmem_limit_bytes=LIMIT),
        name="reduce",
    )(core_part.reshape(n // 2, 2, rows, s), co_part.reshape(n // 2, 2, rows, l))
    range_sketch = range_old + jnp.dot(omega, relaid, preferred_element_type=f32)
    core_sketch = core_old + jnp.dot(phi_all, gathered, preferred_element_type=f32)
    return (range_sketch, corange_sketch, core_sketch)


def solution(mesh):
    placed = (
        P("row", "col"),
        P(None, "row"),
        P(("col", "row"), None),
        P(("col", "row"), None),
        P(None, "row"),
        P(None, ("col", "row")),
        P("row", "col"),
    )
    return jax.shard_map(
        functools.partial(shards, mesh.shape["row"], mesh.shape["col"]),
        mesh=mesh,
        in_specs=placed,
        out_specs=(P(None, ("col", "row")), P("row", "col"), P("row", "col")),
        check_vma=False,
    )
```
